32 devices in a mesh: grp: 2 (over x), gx: 8 (over z, y), gy: 2 (over core).
Axes of the slice: x: 2, y: 2, z: 4, core: 2. Of those that a mesh axis runs over, the one named last changes fastest.
Arguments:
- warmth_anomaly: float32 [64, 128, 256], P('grp', 'gx', 'gy'), may hold values from -6 to 6
- humidity_anomaly: float32 [64, 128, 256], P('grp', 'gx', 'gy'), may hold values from -6 to 6
- horizontal_line_advective_ratio: float32 [64], replicated, may hold values from -0.5 to 0.5
- vertical_line_advective_ratio: float32 [64], replicated, may hold values from -0.5 to 0.5
- molecular_extinction_coefficient: float32 [112], replicated, may hold values from 0.002 to 0.05
- droplet_extinction_thickness: float32 [112], replicated, may hold values from 0.005 to 0.1
- shortwave_quadrature_share: float32 [112], replicated, may hold values from 0.5 to 5
- longwave_quadrature_share: float32 [112], replicated, may hold values from 0.5 to 5
- overcast_layer_flags: int32 [8192, 64], P(('grp', 'gx', 'gy')), may hold values 0 or 1
- profile_position_within_tile: int32 [64, 128], P('gx', 'gy'), may hold values from 0 to 511, as said below
Outputs:
- temperature_out: float32 [64, 128, 256], P('grp', 'gx', 'gy')
- moisture_out: float32 [64, 128, 256], P('grp', 'gx', 'gy')
- warming_rates: float32 [8192, 64], P(('grp', 'gx', 'gy'))
The draws below stay inside these ranges and needn't reach their ends.
Inputs may be any that keep to these rules, and one draw needn't show every extreme that they name: `profile_position_within_tile`: each tile's block of 8 x 64 entries holds every number from 0 to 511 exactly once.
All inputs are finite; a program needn't handle non-finite values. No bound on the sum of `overcast_layer_flags` on one device may be relied on, other than what follows from the above.
Results may differ from the reference program's by a relative error of at most 0.000092.
Values sent between devices are 32-bit elements; how exact they have to be, the bound alone decides.
A program may use at most 64 MiB of HBM per device.

```python
import math
import jax
import jax.numpy as jnp
from jax import lax

VERTICAL_LAYERS = 64
G = 112
SWEEPS = 8
MESH_HEIGHT = 128
MESH_WIDTH = 256
CXC = 8
CYC = 64
NXC = 64
NYC = 128
SLOTS = 512
BATCH_PROFILES = 256
NB = 8192
N_GRP = 2
N_GX = 8
N_GY = 2


def draw_profile_position_within_tile(key, part):
    tiles_x = NXC // CXC
    tiles_y = NYC // CYC
    keys = jax.random.split(key, tiles_x * tiles_y)
    perms = jax.vmap(lambda subkey: jax.random.permutation(subkey, CXC * CYC))(keys)
    perms = perms.reshape(tiles_x, tiles_y, CXC, CYC).transpose(0, 2, 1, 3)
    return perms.reshape(NXC, NYC).astype(jnp.int32)


def set_ends(values, stream_key, least, high):
    longest = values.shape.index(max(values.shape))
    spots = []
    for shift in (0, 1):
        where = [jax.random.randint(jax.random.fold_in(stream_key, axis), (), 0, length) for axis, length in enumerate(values.shape)]
        where[longest] = (where[longest] + shift) % values.shape[longest]
        spots.append(tuple(where))
    return values.at[spots[0]].set(least).at[spots[1]].set(high)


def levels(stream_key, shape, shards, least, high):
    def one(dim, shards_of):
        heights = jax.random.uniform(jax.random.fold_in(jax.random.fold_in(stream_key, 6), dim), (shards_of,), jnp.float32, least / len(shards), high / len(shards))
        return jnp.repeat(jnp.exp(heights), shape[dim] // shards_of).reshape((-1,) + (1,) * (len(shape) - dim - 1))

    gain = one(*shards[0])
    for cut in shards[1:]:
        gain = gain * one(*cut)
    return gain


def gaussian(stream_key, extent, spread, reach, cuts=(), kind=jnp.bfloat16):
    array = spread * jax.random.normal(stream_key, extent, jnp.float32)
    if cuts:
        array = array * levels(stream_key, extent, cuts, -0.22, 0.18)
    return jnp.clip(array, -reach, reach).astype(kind)


def setup_inputs(seed: int = 0) -> dict:
    splits = jax.random.split(jax.random.key(seed), 11)
    warmth_anomaly = gaussian(splits[0], (VERTICAL_LAYERS, MESH_HEIGHT, MESH_WIDTH), 1.0, 6.0, ((0, 2), (1, 8), (2, 2)), jnp.float32)
    humidity_anomaly = gaussian(splits[1], (VERTICAL_LAYERS, MESH_HEIGHT, MESH_WIDTH), 1.0, 6.0, ((0, 2), (1, 8), (2, 2)), jnp.float32)
    horizontal_line_advective_ratio = jnp.clip(jax.random.uniform(splits[2], (VERTICAL_LAYERS,), jnp.float32, -0.5, 0.5), -0.5, 0.5)
    vertical_line_advective_ratio = jnp.clip(jax.random.uniform(splits[3], (VERTICAL_LAYERS,), jnp.float32, -0.5, 0.5), -0.5, 0.5)
    molecular_extinction_coefficient = jnp.clip(jnp.exp(jax.random.uniform(splits[4], (G,), jnp.float32, math.log(0.002), math.log(0.05))), 0.002, 0.05)
    droplet_extinction_thickness = jnp.clip(jnp.exp(jax.random.uniform(splits[5], (G,), jnp.float32, math.log(0.005), math.log(0.1))), 0.005, 0.1)
    shortwave_quadrature_share = jnp.clip(jnp.exp(jax.random.uniform(splits[6], (G,), jnp.float32, math.log(0.5), math.log(5.0))), 0.5, 5.0)
    longwave_quadrature_share = jnp.clip(jnp.exp(jax.random.uniform(splits[7], (G,), jnp.float32, math.log(0.5), math.log(5.0))), 0.5, 5.0)
    overcast_layer_flags = set_ends((jax.random.randint(splits[8], (NB, VERTICAL_LAYERS), 0, 2) < 1).astype(jnp.int32), jax.random.fold_in(splits[8], 1), 0, 1)
    profile_position_within_tile = draw_profile_position_within_tile(jax.random.fold_in(splits[10], 71), 0)
    return dict(warmth_anomaly=warmth_anomaly, humidity_anomaly=humidity_anomaly, horizontal_line_advective_ratio=horizontal_line_advective_ratio, vertical_line_advective_ratio=vertical_line_advective_ratio, molecular_extinction_coefficient=molecular_extinction_coefficient, droplet_extinction_thickness=droplet_extinction_thickness, shortwave_quadrature_share=shortwave_quadrature_share, longwave_quadrature_share=longwave_quadrature_share, overcast_layer_flags=overcast_layer_flags, profile_position_within_tile=profile_position_within_tile)


NU_H = 0.15
NU_V = 0.15
HEATING_INTERVAL = 0.5


def advance_variable(grid_field, horizontal_line_advective_ratio, vertical_line_advective_ratio):
    row_next = jnp.roll(grid_field, -1, 1)
    row_prev = jnp.roll(grid_field, 1, 1)
    col_next = jnp.roll(grid_field, -1, 2)
    col_prev = jnp.roll(grid_field, 1, 2)
    padded = jnp.pad(grid_field, ((1, 1), (0, 0), (0, 0)))
    lev_next = padded[2:]
    lev_prev = padded[:-2]
    speed_x = horizontal_line_advective_ratio[:, None, None]
    speed_y = vertical_line_advective_ratio[:, None, None]
    return (grid_field - 0.5 * speed_x * (row_next - row_prev) - 0.5 * speed_y * (col_next - col_prev)
            + NU_H * (row_next + row_prev + col_next + col_prev - 4.0 * grid_field)
            + NU_V * (lev_next + lev_prev - 2.0 * grid_field))


def reduce_mesh_resolution(grid_field):
    return grid_field.reshape(VERTICAL_LAYERS, NXC, 2, NYC, 2).mean(axis=(2, 4))


def tile_slots(profile_position_within_tile):
    return profile_position_within_tile.reshape(N_GX, CXC, N_GY, CYC).transpose(0, 2, 1, 3).reshape(N_GX, N_GY, SLOTS)


def collect_profiles(coarse, profile_position_within_tile):
    tiles = coarse.reshape(VERTICAL_LAYERS, N_GX, CXC, N_GY, CYC).transpose(1, 3, 2, 4, 0).reshape(N_GX, N_GY, SLOTS, VERTICAL_LAYERS)
    inverse = jnp.argsort(tile_slots(profile_position_within_tile), axis=2).astype(jnp.int32)
    packed = jnp.take_along_axis(tiles, inverse[:, :, :, None], axis=2)
    return packed.reshape(N_GX, N_GY, N_GRP, BATCH_PROFILES, VERTICAL_LAYERS).transpose(2, 0, 1, 3, 4).reshape(NB, VERTICAL_LAYERS)


def unpack_columns(warming_rates, profile_position_within_tile):
    tiles = warming_rates.reshape(N_GRP, N_GX, N_GY, BATCH_PROFILES, VERTICAL_LAYERS).transpose(1, 2, 0, 3, 4).reshape(N_GX, N_GY, SLOTS, VERTICAL_LAYERS)
    placed = jnp.take_along_axis(tiles, tile_slots(profile_position_within_tile)[:, :, :, None], axis=2)
    return placed.reshape(N_GX, N_GY, CXC, CYC, VERTICAL_LAYERS).transpose(4, 0, 2, 1, 3).reshape(VERTICAL_LAYERS, NXC, NYC)


def refine_heat(coarse):
    even_rows = 0.75 * coarse + 0.25 * jnp.roll(coarse, 1, 1)
    odd_rows = 0.75 * coarse + 0.25 * jnp.roll(coarse, -1, 1)
    rows_done = jnp.stack([even_rows, odd_rows], axis=2).reshape(VERTICAL_LAYERS, MESH_HEIGHT, NYC)
    even_cols = 0.75 * rows_done + 0.25 * jnp.roll(rows_done, 1, 2)
    odd_cols = 0.75 * rows_done + 0.25 * jnp.roll(rows_done, -1, 2)
    return jnp.stack([even_cols, odd_cols], axis=3).reshape(VERTICAL_LAYERS, MESH_HEIGHT, MESH_WIDTH)


def radiate(theta_rows, moist_rows, mask_rows, molecular_extinction_coefficient, droplet_extinction_thickness, shortwave_quadrature_share, longwave_quadrature_share):
    absorber = jax.nn.softplus(moist_rows)
    cloudy = mask_rows.astype(jnp.float32)
    optical_depth = absorber[:, :, None] * molecular_extinction_coefficient + cloudy[:, :, None] * droplet_extinction_thickness
    optical_path_above = jnp.cumsum(optical_depth, axis=1) - optical_depth
    absorbed = 1.0 - jnp.exp(-optical_depth)
    shortwave_total = jnp.sum(shortwave_quadrature_share * jnp.exp(-optical_path_above) * absorbed, axis=2)
    longwave_total = jnp.sum(longwave_quadrature_share * absorbed, axis=2)
    return (shortwave_total - longwave_total * (1.0 + 0.1 * theta_rows)) * (4.0 / G)


def reference(warmth_anomaly, humidity_anomaly, horizontal_line_advective_ratio, vertical_line_advective_ratio, molecular_extinction_coefficient, droplet_extinction_thickness, shortwave_quadrature_share, longwave_quadrature_share, overcast_layer_flags, profile_position_within_tile):
    theta_vertical_profile = collect_profiles(reduce_mesh_resolution(warmth_anomaly), profile_position_within_tile)
    humidity_profile = collect_profiles(reduce_mesh_resolution(humidity_anomaly), profile_position_within_tile)
    partitions = NB // BATCH_PROFILES

    def within_partition(items):
        return radiate(items[0], items[1], items[2], molecular_extinction_coefficient, droplet_extinction_thickness, shortwave_quadrature_share, longwave_quadrature_share)

    warming_rates = lax.map(within_partition, (theta_vertical_profile.reshape(partitions, BATCH_PROFILES, VERTICAL_LAYERS), humidity_profile.reshape(partitions, BATCH_PROFILES, VERTICAL_LAYERS),
                                  overcast_layer_flags.reshape(partitions, BATCH_PROFILES, VERTICAL_LAYERS))).reshape(NB, VERTICAL_LAYERS)
    warming_refined = refine_heat(unpack_columns(warming_rates, profile_position_within_tile))
    present_heat_anomaly = warmth_anomaly
    humidity_present = humidity_anomaly
    for sweep_index in range(SWEEPS):
        present_heat_anomaly = advance_variable(present_heat_anomaly, horizontal_line_advective_ratio, vertical_line_advective_ratio)
        humidity_present = advance_variable(humidity_present, horizontal_line_advective_ratio, vertical_line_advective_ratio)
    return present_heat_anomaly + HEATING_INTERVAL * warming_refined, humidity_present, warming_rates
```

```python
import functools
import math

import jax
import jax.numpy as jnp
from jax import lax
from jax.experimental import pallas as pl
from jax.experimental.pallas import tpu as pltpu
from jax.sharding import PartitionSpec as P

SWEEPS = 8
NU_H = 0.15
NU_V = 0.15
HEATING_INTERVAL = 0.5
M = 8
MESH = pl.DeviceIdType.MESH
BF = jnp.bfloat16
F32 = jnp.float32


def split_bf16(x):
    hi = x.astype(BF)
    lo = (x - hi.astype(F32)).astype(BF)
    return hi, lo


def kernel(
    n_gx, n_gy, L, R, C, S, B, G,
    warm_in, humid_in, cx_ref, cy_ref, gas_ref, drop_ref, sw_ref, lw_ref, flags_ref, slot_ref,
    t_out, m_out, rates_out,
    ext, edge_send, edge_recv, qt, packed, rad, coef, cloudy, absorber, theta, rates, heat, ucols,
    hedge_send, hedge_recv, rows_send, rows_recv,
    halo_send_sem, halo_recv_sem, edge_send_sem, edge_recv_sem, misc_send_sem, misc_recv_sem,
):
    g = lax.axis_index("grp")
    x = lax.axis_index("gx")
    y = lax.axis_index("gy")
    og = 1 - g
    xn, xp = lax.rem(x + 1, n_gx), lax.rem(x + n_gx - 1, n_gx)
    yn, yp = lax.rem(y + 1, n_gy), lax.rem(y + n_gy - 1, n_gy)
    fields = (warm_in, humid_in)
    outs = (t_out, m_out)
    LE = L + M
    T = (R + 2 * M) // 8
    per = C // T
    NP = -(-LE // per)
    RI = R // 2
    RLO = 8
    ROWN = RLO + M
    RE = R + 2 * M

    barrier = pltpu.get_barrier_semaphore()
    for dev in ((g, xn, y), (g, xp, y), (og, x, y), (og, xn, y), (og, xp, y), (g, x, yn), (g, x, yp)):
        pl.semaphore_signal(barrier, inc=1, device_id=dev, device_id_type=MESH)
    pl.semaphore_wait(barrier, 7)

    def remote(src, dst, ss, rs, dev):
        c = pltpu.make_async_remote_copy(
            src_ref=src, dst_ref=dst, send_sem=ss, recv_sem=rs, device_id=dev, device_id_type=MESH
        )
        c.start()
        return c

    half = slot_ref.shape[1]
    slots = slot_ref[...]
    rep = (
        lax.broadcasted_iota(jnp.int32, (half, C), 1) // 2
        == lax.broadcasted_iota(jnp.int32, (half, C), 0)
    ).astype(F32).astype(BF)
    s_hi = (slots // 16).astype(F32).astype(BF)
    s_lo = (slots % 16).astype(F32).astype(BF)
    slot_rep = (
        16.0 * jnp.dot(s_hi, rep, preferred_element_type=F32)
        + jnp.dot(s_lo, rep, preferred_element_type=F32)
    ).astype(jnp.int32)
    s_iota = lax.broadcasted_iota(jnp.int32, (S, C), 0)
    for i in range(RI):
        qt[:, i * C : (i + 1) * C] = jnp.where(s_iota == slot_rep[i : i + 1, :], 1.0, 0.0).astype(BF)
    parts = []
    for i in range(RI):
        col = []
        for f in range(2):
            flat = fields[f].reshape(L * R, C)
            col.append(
                flat[pl.ds(2 * i, L, stride=R), :] + flat[pl.ds(2 * i + 1, L, stride=R), :]
            )
        hi, lo = split_bf16(0.25 * jnp.concatenate(col, axis=0))
        parts.append(jnp.concatenate([hi, lo], axis=0))
    lhs = jnp.concatenate(parts, axis=1)
    both = lax.dot_general(
        lhs, qt[...], (((1,), (1,)), ((), ())), preferred_element_type=F32
    )
    both = both[: 2 * L] + both[2 * L :]
    for h in range(2):
        packed[h] = both[:, h * B : (h + 1) * B]
    c_packed = remote(packed.at[og], rad.at[g], misc_send_sem.at[0], misc_recv_sem.at[0], (og, x, y))

    lev_src = (L - M) * og
    lev_dst = 1 + L * g
    own_dst = 1 + M * g
    halos = []
    n = 0
    for f in range(2):
        for levs, dlevs, count, gg in ((0, own_dst, L, g), (lev_src, lev_dst, M, og)):
            for r0, d0, xx in ((R - M, RLO, xn), (0, ROWN + R, xp)):
                halos.append(remote(
                    fields[f].at[pl.ds(levs, count), r0 : r0 + M, :],
                    ext.at[0, f, pl.ds(dlevs, count), d0 : d0 + M, :],
                    halo_send_sem.at[n], halo_recv_sem.at[n], (gg, xx, y),
                ))
                n += 1
        halos.append(remote(
            fields[f].at[pl.ds(lev_src, M)],
            ext.at[0, f, pl.ds(lev_dst, M), ROWN : ROWN + R, :],
            halo_send_sem.at[n], halo_recv_sem.at[n], (og, x, y),
        ))
        n += 1
    rad[g] = packed[g]
    for f in range(2):
        ext[0, f, pl.ds(own_dst, L), ROWN : ROWN + R, :] = fields[f][...]
        for b in range(2):
            for p in (0, LE + 1):
                ext[b, f, p] = jnp.zeros_like(ext[b, f, p])

    log2e = 1.0 / math.log(2.0)
    for q, (ref, scale) in enumerate(((gas_ref, -log2e), (drop_ref, -log2e), (sw_ref, 1.0), (lw_ref, 1.0))):
        coef[q] = jnp.broadcast_to(ref[...] * scale, (128, G)).T
    for hb in range(B // 128):
        cloudy[hb] = flags_ref[hb * 128 : (hb + 1) * 128, :].astype(F32).T

    c_packed.wait()
    for o in range(2):
        mo = rad[o, L : 2 * L, :]
        soft = jnp.maximum(mo, 0.0) + jnp.log1p(jnp.exp(-jnp.abs(mo)))
        for hb in range(B // 128):
            absorber[hb, o * L : (o + 1) * L, :] = soft[:, hb * 128 : (hb + 1) * 128]
            theta[hb, o * L : (o + 1) * L, :] = rad[o, 0:L, hb * 128 : (hb + 1) * 128]

    GB = G // 8
    norm = 4.0 / G
    for hb in range(B // 128):
        for o in range(2):
            def level(l, flux, o=o, hb=hb):
                lg = l + o * L
                a = jnp.broadcast_to(absorber[hb, pl.ds(lg, 1), :], (8, 128))
                c = jnp.broadcast_to(cloudy[hb, pl.ds(lg, 1), :], (8, 128))
                th = 1.0 + 0.1 * theta[hb, pl.ds(lg, 1), :]
                sw = lw = None
                new = []
                for q in range(GB):
                    rows = slice(8 * q, 8 * q + 8)
                    d = 1.0 - jnp.exp2(a * coef[0, rows, :] + c * coef[1, rows, :])
                    s = flux[q] * d
                    w = coef[3, rows, :] * d
                    sw = s if sw is None else sw + s
                    lw = w if lw is None else lw + w
                    new.append(flux[q] - s)
                total = jnp.sum(sw - lw * th, axis=0, keepdims=True) * norm
                rates[o, hb, pl.ds(l, 1), :] = total
                return tuple(new)

            if o == 0:
                flux = tuple(coef[2, 8 * q : 8 * q + 8, :] for q in range(GB))
            flux = lax.fori_loop(0, L, level, flux, unroll=2)
    c_heat = remote(rates.at[og], heat.at[g], misc_send_sem.at[1], misc_recv_sem.at[1], (og, x, y))
    heat[g] = rates[g]
    for o in range(2):
        for hb in range(B // 128):
            rates_out[hb * 128 : (hb + 1) * 128, o * L : (o + 1) * L] = rates[o, hb].T

    lane = lax.broadcasted_iota(jnp.int32, (8, C), 1)

    def pack(vals, j, accs):
        right, left = accs
        for t in range(T):
            k = j * T + t
            turned = pltpu.roll(vals[8 * t : 8 * t + 8, :], lax.rem(k + 1, C), 1)
            right = jnp.where(lane == k, turned, right)
            left = jnp.where(lane == lax.rem(k + 1, C), turned, left)
        return right, left

    def send_edges(k, f):
        return (
            remote(edge_send.at[k, f, 0], edge_recv.at[k, f, 0],
                   edge_send_sem.at[k, f, 0], edge_recv_sem.at[k, f, 0], (g, x, yn)),
            remote(edge_send.at[k, f, 1], edge_recv.at[k, f, 1],
                   edge_send_sem.at[k, f, 1], edge_recv_sem.at[k, f, 1], (g, x, yp)),
        )

    zero = jnp.zeros((8, C), F32)

    def run_levels(k, f, count, values):
        for p in range(NP):
            lo, hi = p * per, min(count, (p + 1) * per)
            if lo >= hi:
                edge_send[k, f, 0, p] = zero
                edge_send[k, f, 1, p] = zero
                continue
            right, left = lax.fori_loop(
                lo, hi, lambda j, accs, lo=lo: pack(values(j), j - lo, accs), (zero, zero), unroll=2
            )
            edge_send[k, f, 0, p] = right
            edge_send[k, f, 1, p] = left

    def first(f):
        run_levels(0, f, LE, lambda j: ext[0, f, j + 1, RLO : RLO + RE, :])
        return send_edges(0, f)

    def sweep(k, f):
        src, dst = (k - 1) % 2, k % 2
        start = g * k
        last = k == SWEEPS
        t0, t1 = (M // 8, M // 8 + R // 8) if last else (0, T)
        r0, r1 = RLO + 8 * t0, RLO + 8 * t1

        def values(j):
            lev = start + j
            p = lev + 1
            jj = j + g
            which = jj // per
            kk = (jj - which * per) * T
            from_left = edge_recv[k - 1, f, 0, which]
            from_right = edge_recv[k - 1, f, 1, which]
            lg = lev + (L - M) * g
            sx = 0.5 * cx_ref[lg]
            sy = 0.5 * cy_ref[lg]
            cen = ext[src, f, p, r0:r1, :]
            base = (
                (1.0 - 4.0 * NU_H - 2.0 * NU_V) * cen
                + NU_V * (ext[src, f, p + 1, r0:r1, :] + ext[src, f, p - 1, r0:r1, :])
                + (NU_H - sx) * ext[src, f, p, r0 + 1 : r1 + 1, :]
                + (NU_H + sx) * ext[src, f, p, r0 - 1 : r1 - 1, :]
            )
            res = []
            for t in range(t0, t1):
                q = 8 * (t - t0)
                v = cen[q : q + 8, :]
                kt = kk + t
                prev = jnp.where(lane == 0, pltpu.roll(from_left, lax.rem(C - kt, C), 1), pltpu.roll(v, 1, 1))
                nxt = jnp.where(
                    lane == C - 1, pltpu.roll(from_right, lax.rem(2 * C - 2 - kt, C), 1), pltpu.roll(v, C - 1, 1)
                )
                res.append(base[q : q + 8, :] + (NU_H - sy) * nxt + (NU_H + sy) * prev)
            new = jnp.concatenate(res, axis=0)
            if last:
                outs[f][j] = new
            else:
                ext[dst, f, p, RLO : RLO + RE, :] = new
            return new

        count = LE - k
        if last:
            @pl.loop(0, count, unroll=2)
            def _(j):
                values(j)
            return None
        run_levels(k, f, count, values)
        return send_edges(k, f)

    for c in halos:
        c.wait()
    flight = [first(0), first(1)]
    sent = []

    def advance(ks):
        for k in ks:
            for f in range(2):
                for c in flight[f]:
                    c.wait()
                flight[f] = sweep(k, f)

    advance((1, 2))

    c_heat.wait()
    hi, lo = split_bf16(jnp.concatenate([heat[h, hb] for h in range(2) for hb in range(B // 128)], axis=1))
    spread = jnp.dot(jnp.concatenate([hi, lo], axis=0), qt[...], preferred_element_type=F32)
    spread = spread[:L] + spread[L:]
    LT = L // 8
    ehi = zero
    elo = zero
    for i in range(RI):
        ui = spread[:, i * C : (i + 1) * C]
        ucols[i] = ui
        for t in range(LT):
            k = i * LT + t
            turned = pltpu.roll(ui[8 * t : 8 * t + 8, :], (k + 1) % C, 1)
            ehi = jnp.where(lane == k, turned, ehi)
            elo = jnp.where(lane == (k + 1) % C, turned, elo)
    hedge_send[0] = ehi
    hedge_send[1] = elo
    c_he = [
        remote(hedge_send.at[0], hedge_recv.at[0], misc_send_sem.at[2], misc_recv_sem.at[2], (g, x, yn)),
        remote(hedge_send.at[1], hedge_recv.at[1], misc_send_sem.at[3], misc_recv_sem.at[3], (g, x, yp)),
    ]
    advance((3,))
    for c in c_he:
        c.wait()
    from_left = hedge_recv[0]
    from_right = hedge_recv[1]
    even = lane % 2 == 0
    for i in range(RI):
        for t in range(LT):
            k = i * LT + t
            v = ucols[i, 8 * t : 8 * t + 8, :]
            prev = jnp.where(lane == 0, pltpu.roll(from_left, (C - k) % C, 1), pltpu.roll(v, 1, 1))
            nxt = jnp.where(lane == C - 1, pltpu.roll(from_right, (2 * C - 2 - k) % C, 1), pltpu.roll(v, C - 1, 1))
            w = 0.75 * v + 0.25 * jnp.where(even, prev, nxt)
            ucols[i, 8 * t : 8 * t + 8, :] = w
            if i == 0:
                rows_send[0, 8 * t : 8 * t + 8, :] = w
            if i == RI - 1:
                rows_send[1, 8 * t : 8 * t + 8, :] = w
    c_rows = [
        remote(rows_send.at[0], rows_recv.at[0], misc_send_sem.at[4], misc_recv_sem.at[4], (g, xp, y)),
        remote(rows_send.at[1], rows_recv.at[1], misc_send_sem.at[5], misc_recv_sem.at[5], (g, xn, y)),
    ]
    advance(range(4, SWEEPS + 1))
    for c in c_rows:
        c.wait()
    flat = t_out.reshape(L * R, C)
    for i in range(RI):
        v = ucols[i]
        above = rows_recv[1] if i == 0 else ucols[i - 1]
        below = rows_recv[0] if i == RI - 1 else ucols[i + 1]
        flat[pl.ds(2 * i, L, stride=R), :] = flat[pl.ds(2 * i, L, stride=R), :] + HEATING_INTERVAL * (0.75 * v + 0.25 * above)
        flat[pl.ds(2 * i + 1, L, stride=R), :] = flat[pl.ds(2 * i + 1, L, stride=R), :] + HEATING_INTERVAL * (0.75 * v + 0.25 * below)


def body(n_gx, n_gy, warm, humid, cx, cy, gas, drop, sw, lw, flags, slots):
    L, R, C = warm.shape
    S = slots.shape[0] * slots.shape[1]
    B = flags.shape[0]
    G = gas.shape[0]
    LE = L + M
    T = (R + 2 * M) // 8
    NP = -(-LE // (C // T))
    vmem = pl.BlockSpec(memory_space=pltpu.VMEM)
    smem = pl.BlockSpec(memory_space=pltpu.SMEM)
    return pl.pallas_call(
        functools.partial(kernel, n_gx, n_gy, L, R, C, S, B, G),
        out_shape=(
            jax.ShapeDtypeStruct((L, R, C), F32),
            jax.ShapeDtypeStruct((L, R, C), F32),
            jax.ShapeDtypeStruct((B, 2 * L), F32),
        ),
        in_specs=[vmem, vmem, smem, smem] + [vmem] * 6,
        out_specs=(vmem, vmem, vmem),
        scratch_shapes=[
            pltpu.VMEM((2, 2, LE + 2, R + 2 * M + 16, C), F32),
            pltpu.VMEM((SWEEPS, 2, 2, NP, 8, C), F32),
            pltpu.VMEM((SWEEPS, 2, 2, NP, 8, C), F32),
            pltpu.VMEM((S, (R // 2) * C), BF),
            pltpu.VMEM((2, 2 * L, B), F32),
            pltpu.VMEM((2, 2 * L, B), F32),
            pltpu.VMEM((4, G, 128), F32),
            pltpu.VMEM((B // 128, 2 * L, 128), F32),
            pltpu.VMEM((B // 128, 2 * L, 128), F32),
            pltpu.VMEM((B // 128, 2 * L, 128), F32),
            pltpu.VMEM((2, B // 128, L, 128), F32),
            pltpu.VMEM((2, B // 128, L, 128), F32),
            pltpu.VMEM((R // 2, L, C), F32),
            pltpu.VMEM((2, 8, C), F32),
            pltpu.VMEM((2, 8, C), F32),
            pltpu.VMEM((2, L, C), F32),
            pltpu.VMEM((2, L, C), F32),
            pltpu.SemaphoreType.DMA((10,)),
            pltpu.SemaphoreType.DMA((10,)),
            pltpu.SemaphoreType.DMA((SWEEPS, 2, 2)),
            pltpu.SemaphoreType.DMA((SWEEPS, 2, 2)),
            pltpu.SemaphoreType.DMA((6,)),
            pltpu.SemaphoreType.DMA((6,)),
        ],
        compiler_params=pltpu.CompilerParams(collective_id=0, has_side_effects=True),
    )(
        warm, humid, cx, cy, gas[None], drop[None], sw[None], lw[None], flags, slots,
    )


def solution(mesh):
    assert mesh.shape["grp"] == 2
    in_specs = (
        P("grp", "gx", "gy"), P("grp", "gx", "gy"), P(), P(), P(), P(), P(), P(),
        P(("grp", "gx", "gy"), None), P("gx", "gy"),
    )
    out_specs = (P("grp", "gx", "gy"), P("grp", "gx", "gy"), P(("grp", "gx", "gy"), None))
    return jax.shard_map(
        functools.partial(body, mesh.shape["gx"], mesh.shape["gy"]),
        mesh=mesh, in_specs=in_specs, out_specs=out_specs, check_vma=False,
    )
```

```python
import functools
import math

import jax
import jax.numpy as jnp
from jax import lax
from jax.experimental import pallas as pl
from jax.experimental.pallas import tpu as pltpu
from jax.sharding import PartitionSpec as P

SWEEPS = 8
NU_H = 0.15
NU_V = 0.15
HEATING_INTERVAL = 0.5
UNROLL = 8
M = 8
MESH = pl.DeviceIdType.MESH
BF = jnp.bfloat16
F32 = jnp.float32


def split_bf16(x):
    hi = x.astype(BF)
    lo = (x - hi.astype(F32)).astype(BF)
    return hi, lo


def kernel(
    n_gx, n_gy, L, R, C, S, B, G,
    warm_in, humid_in, cx_ref, cy_ref, gas_ref, drop_ref, sw_ref, lw_ref, flags_ref, slot_ref,
    t_out, m_out, rates_out,
    ext0, ext1, edge_send, edge_recv, qt, packed, rad, coef, cloudy, absorber, theta, rates, heat, ucols,
    hedge_send, hedge_recv, rows_send, rows_recv,
    halo_send_sem, halo_recv_sem, edge_send_sem, edge_recv_sem, misc_send_sem, misc_recv_sem,
):
    g = lax.axis_index("grp")
    x = lax.axis_index("gx")
    y = lax.axis_index("gy")
    og = 1 - g
    xn, xp = lax.rem(x + 1, n_gx), lax.rem(x + n_gx - 1, n_gx)
    yn, yp = lax.rem(y + 1, n_gy), lax.rem(y + n_gy - 1, n_gy)
    fields = (warm_in, humid_in)
    ext = (ext0, ext1)
    outs = (t_out, m_out)
    LE = L + M
    T = (R + 2 * M) // 8
    per = C // T
    NP = -(-LE // per)
    RI = R // 2
    RLO = 8
    ROWN = RLO + M
    RE = R + 2 * M

    barrier = pltpu.get_barrier_semaphore()
    for dev in ((g, xn, y), (g, xp, y), (og, x, y), (og, xn, y), (og, xp, y), (g, x, yn), (g, x, yp)):
        pl.semaphore_signal(barrier, inc=1, device_id=dev, device_id_type=MESH)
    pl.semaphore_wait(barrier, 7)

    def remote(src, dst, ss, rs, dev):
        c = pltpu.make_async_remote_copy(
            src_ref=src, dst_ref=dst, send_sem=ss, recv_sem=rs, device_id=dev, device_id_type=MESH
        )
        c.start()
        return c

    half = slot_ref.shape[1]
    slots = slot_ref[...]
    rep = (
        lax.broadcasted_iota(jnp.int32, (half, C), 1) // 2
        == lax.broadcasted_iota(jnp.int32, (half, C), 0)
    ).astype(F32).astype(BF)
    s_hi = (slots // 16).astype(F32).astype(BF)
    s_lo = (slots % 16).astype(F32).astype(BF)
    slot_rep = (
        16.0 * jnp.dot(s_hi, rep, preferred_element_type=F32)
        + jnp.dot(s_lo, rep, preferred_element_type=F32)
    ).astype(jnp.int32)
    s_iota = lax.broadcasted_iota(jnp.int32, (S, C), 0)
    for i in range(RI):
        qt[:, i * C : (i + 1) * C] = jnp.where(s_iota == slot_rep[i : i + 1, :], 1.0, 0.0).astype(BF)
    parts = []
    for i in range(RI):
        col = []
        for f in range(2):
            flat = fields[f].reshape(L * R, C)
            col.append(
                flat[pl.ds(2 * i, L, stride=R), :] + flat[pl.ds(2 * i + 1, L, stride=R), :]
            )
        hi, lo = split_bf16(0.25 * jnp.concatenate(col, axis=0))
        parts.append(jnp.concatenate([hi, lo], axis=0))
    lhs = jnp.concatenate(parts, axis=1)
    both = lax.dot_general(
        lhs, qt[...], (((1,), (1,)), ((), ())), preferred_element_type=F32
    )
    both = both[: 2 * L] + both[2 * L :]
    for h in range(2):
        packed[h] = both[:, h * B : (h + 1) * B]
    c_packed = remote(packed.at[og], rad.at[g], misc_send_sem.at[0], misc_recv_sem.at[0], (og, x, y))

    lev_src = (L - M) * og
    lev_dst = 1 + L * g
    own_dst = 1 + M * g
    halos = []
    n = 0
    for f in range(2):
        for levs, dlevs, count, gg in ((0, own_dst, L, g), (lev_src, lev_dst, M, og)):
            for r0, d0, xx in ((R - M, RLO, xn), (0, ROWN + R, xp)):
                halos.append(remote(
                    fields[f].at[pl.ds(levs, count), r0 : r0 + M, :],
                    ext0.at[f, pl.ds(dlevs, count), d0 : d0 + M, :],
                    halo_send_sem.at[n], halo_recv_sem.at[n], (gg, xx, y),
                ))
                n += 1
        halos.append(remote(
            fields[f].at[pl.ds(lev_src, M)],
            ext0.at[f, pl.ds(lev_dst, M), ROWN : ROWN + R, :],
            halo_send_sem.at[n], halo_recv_sem.at[n], (og, x, y),
        ))
        n += 1
    rad[g] = packed[g]
    for f in range(2):
        ext0[f, pl.ds(own_dst, L), ROWN : ROWN + R, :] = fields[f][...]
        for b in range(2):
            for p in (0, LE + 1):
                ext[b][f, p] = jnp.zeros((RE + 16, C), F32)

    log2e = 1.0 / math.log(2.0)
    for q, (ref, scale) in enumerate(((gas_ref, -log2e), (drop_ref, -log2e), (sw_ref, 1.0), (lw_ref, 1.0))):
        coef[q] = jnp.broadcast_to(ref[...] * scale, (128, G)).T
    for hb in range(B // 128):
        cloudy[hb] = flags_ref[:, hb * 128 : (hb + 1) * 128].astype(F32)

    c_packed.wait()
    for o in range(2):
        mo = rad[o, L : 2 * L, :]
        soft = jnp.maximum(mo, 0.0) + jnp.log1p(jnp.exp(-jnp.abs(mo)))
        for hb in range(B // 128):
            absorber[hb, o * L : (o + 1) * L, :] = soft[:, hb * 128 : (hb + 1) * 128]
            theta[hb, o * L : (o + 1) * L, :] = rad[o, 0:L, hb * 128 : (hb + 1) * 128]

    GB = G // 8
    norm = 4.0 / G
    for hb in range(B // 128):
        for o in range(2):
            def level(l, flux, o=o, hb=hb):
                lg = l + o * L
                a = jnp.broadcast_to(absorber[hb, pl.ds(lg, 1), :], (8, 128))
                c = jnp.broadcast_to(cloudy[hb, pl.ds(lg, 1), :], (8, 128))
                th = 1.0 + 0.1 * theta[hb, pl.ds(lg, 1), :]
                sw = lw = None
                new = []
                for q in range(GB):
                    rows = slice(8 * q, 8 * q + 8)
                    d = 1.0 - jnp.exp2(a * coef[0, rows, :] + c * coef[1, rows, :])
                    s = flux[q] * d
                    w = coef[3, rows, :] * d
                    sw = s if sw is None else sw + s
                    lw = w if lw is None else lw + w
                    new.append(flux[q] - s)
                total = jnp.sum(sw - lw * th, axis=0, keepdims=True) * norm
                rates[o, hb, pl.ds(l, 1), :] = total
                return tuple(new)

            if o == 0:
                flux = tuple(coef[2, 8 * q : 8 * q + 8, :] for q in range(GB))
            flux = lax.fori_loop(0, L, level, flux, unroll=2)
    c_heat = remote(rates.at[og], heat.at[g], misc_send_sem.at[1], misc_recv_sem.at[1], (og, x, y))
    heat[g] = rates[g]
    for o in range(2):
        for hb in range(B // 128):
            rates_out[o * L : (o + 1) * L, hb * 128 : (hb + 1) * 128] = rates[o, hb]

    lane = lax.broadcasted_iota(jnp.int32, (8, C), 1)

    def pack(vals, j, accs):
        right, left = accs
        for t in range(T):
            k = j * T + t
            turned = pltpu.roll(vals[8 * t : 8 * t + 8, :], lax.rem(k + 1, C), 1)
            right = jnp.where(lane == k, turned, right)
            left = jnp.where(lane == lax.rem(k + 1, C), turned, left)
        return right, left

    def send_edges(k, f):
        return (
            remote(edge_send.at[k, f, 0], edge_recv.at[k, f, 0],
                   edge_send_sem.at[k, f, 0], edge_recv_sem.at[k, f, 0], (g, x, yn)),
            remote(edge_send.at[k, f, 1], edge_recv.at[k, f, 1],
                   edge_send_sem.at[k, f, 1], edge_recv_sem.at[k, f, 1], (g, x, yp)),
        )

    zero = jnp.zeros((8, C), F32)

    def run_levels(k, f, count, values):
        for p in range(NP):
            lo, hi = p * per, min(count, (p + 1) * per)
            if lo >= hi:
                edge_send[k, f, 0, p] = zero
                edge_send[k, f, 1, p] = zero
                continue
            right, left = lax.fori_loop(
                lo, hi, lambda j, accs, lo=lo: pack(values(j), j - lo, accs), (zero, zero),
                unroll=min(UNROLL, hi - lo),
            )
            edge_send[k, f, 0, p] = right
            edge_send[k, f, 1, p] = left

    def first(f):
        run_levels(0, f, LE, lambda j: ext0[f, j + 1, RLO : RLO + RE, :])
        return send_edges(0, f)

    def sweep(k, f):
        src, dst = (k - 1) % 2, k % 2
        start = g * k
        last = k == SWEEPS
        t0, t1 = (M // 8, M // 8 + R // 8) if last else (0, T)
        r0, r1 = RLO + 8 * t0, RLO + 8 * t1

        def values(j):
            lev = start + j
            p = lev + 1
            jj = j + g
            which = jj // per
            kk = (jj - which * per) * T
            from_left = edge_recv[k - 1, f, 0, which]
            from_right = edge_recv[k - 1, f, 1, which]
            lg = lev + (L - M) * g
            sx = 0.5 * cx_ref[lg]
            sy = 0.5 * cy_ref[lg]
            cen = ext[src][f, p, r0:r1, :]
            base = (
                (1.0 - 4.0 * NU_H - 2.0 * NU_V) * cen
                + NU_V * (ext[src][f, p + 1, r0:r1, :] + ext[src][f, p - 1, r0:r1, :])
                + (NU_H - sx) * ext[src][f, p, r0 + 1 : r1 + 1, :]
                + (NU_H + sx) * ext[src][f, p, r0 - 1 : r1 - 1, :]
            )
            res = []
            for t in range(t0, t1):
                q = 8 * (t - t0)
                v = cen[q : q + 8, :]
                kt = kk + t
                prev = jnp.where(lane == 0, pltpu.roll(from_left, lax.rem(C - kt, C), 1), pltpu.roll(v, 1, 1))
                nxt = jnp.where(
                    lane == C - 1, pltpu.roll(from_right, lax.rem(2 * C - 2 - kt, C), 1), pltpu.roll(v, C - 1, 1)
                )
                res.append(base[q : q + 8, :] + (NU_H - sy) * nxt + (NU_H + sy) * prev)
            new = jnp.concatenate(res, axis=0)
            if last:
                outs[f][j] = new
            else:
                ext[dst][f, p, RLO : RLO + RE, :] = new
            return new

        count = LE - k
        if last:
            @pl.loop(0, count, unroll=UNROLL)
            def _(j):
                values(j)
            return None
        run_levels(k, f, count, values)
        return send_edges(k, f)

    for c in halos:
        c.wait()
    flight = [first(0), first(1)]
    sent = []

    def advance(ks):
        for k in ks:
            for f in range(2):
                for c in flight[f]:
                    c.wait()
                flight[f] = sweep(k, f)

    advance((1, 2))

    c_heat.wait()
    hi, lo = split_bf16(jnp.concatenate([heat[h, hb] for h in range(2) for hb in range(B // 128)], axis=1))
    spread = jnp.dot(jnp.concatenate([hi, lo], axis=0), qt[...], preferred_element_type=F32)
    spread = spread[:L] + spread[L:]
    LT = L // 8
    ehi = zero
    elo = zero
    for i in range(RI):
        ui = spread[:, i * C : (i + 1) * C]
        ucols[i] = ui
        for t in range(LT):
            k = i * LT + t
            turned = pltpu.roll(ui[8 * t : 8 * t + 8, :], (k + 1) % C, 1)
            ehi = jnp.where(lane == k, turned, ehi)
            elo = jnp.where(lane == (k + 1) % C, turned, elo)
    hedge_send[0] = ehi
    hedge_send[1] = elo
    c_he = [
        remote(hedge_send.at[0], hedge_recv.at[0], misc_send_sem.at[2], misc_recv_sem.at[2], (g, x, yn)),
        remote(hedge_send.at[1], hedge_recv.at[1], misc_send_sem.at[3], misc_recv_sem.at[3], (g, x, yp)),
    ]
    advance((3,))
    for c in c_he:
        c.wait()
    from_left = hedge_recv[0]
    from_right = hedge_recv[1]
    even = lane % 2 == 0
    for i in range(RI):
        for t in range(LT):
            k = i * LT + t
            v = ucols[i, 8 * t : 8 * t + 8, :]
            prev = jnp.where(lane == 0, pltpu.roll(from_left, (C - k) % C, 1), pltpu.roll(v, 1, 1))
            nxt = jnp.where(lane == C - 1, pltpu.roll(from_right, (2 * C - 2 - k) % C, 1), pltpu.roll(v, C - 1, 1))
            w = 0.75 * v + 0.25 * jnp.where(even, prev, nxt)
            ucols[i, 8 * t : 8 * t + 8, :] = w
            if i == 0:
                rows_send[0, 8 * t : 8 * t + 8, :] = w
            if i == RI - 1:
                rows_send[1, 8 * t : 8 * t + 8, :] = w
    c_rows = [
        remote(rows_send.at[0], rows_recv.at[0], misc_send_sem.at[4], misc_recv_sem.at[4], (g, xp, y)),
        remote(rows_send.at[1], rows_recv.at[1], misc_send_sem.at[5], misc_recv_sem.at[5], (g, xn, y)),
    ]
    advance(range(4, SWEEPS + 1))
    for c in c_rows:
        c.wait()
    flat = t_out.reshape(L * R, C)
    for i in range(RI):
        v = ucols[i]
        above = rows_recv[1] if i == 0 else ucols[i - 1]
        below = rows_recv[0] if i == RI - 1 else ucols[i + 1]
        flat[pl.ds(2 * i, L, stride=R), :] = flat[pl.ds(2 * i, L, stride=R), :] + HEATING_INTERVAL * (0.75 * v + 0.25 * above)
        flat[pl.ds(2 * i + 1, L, stride=R), :] = flat[pl.ds(2 * i + 1, L, stride=R), :] + HEATING_INTERVAL * (0.75 * v + 0.25 * below)


def hand_on(t_in, m_in, r_in, t_out, m_out, r_out):
    t_out[...] = t_in[...]
    m_out[...] = m_in[...]
    r_out[...] = r_in[...]


def body(n_gx, n_gy, warm, humid, cx, cy, gas, drop, sw, lw, flags, slots):
    L, R, C = warm.shape
    S = slots.shape[0] * slots.shape[1]
    B = flags.shape[0]
    flags = flags.T
    G = gas.shape[0]
    LE = L + M
    T = (R + 2 * M) // 8
    NP = -(-LE // (C // T))
    vmem = pl.BlockSpec(memory_space=pltpu.VMEM)
    smem = pl.BlockSpec(memory_space=pltpu.SMEM)
    t, m, rates = pl.pallas_call(
        functools.partial(kernel, n_gx, n_gy, L, R, C, S, B, G),
        out_shape=(
            jax.ShapeDtypeStruct((L, R, C), F32),
            jax.ShapeDtypeStruct((L, R, C), F32),
            jax.ShapeDtypeStruct((2 * L, B), F32),
        ),
        in_specs=[vmem, vmem, smem, smem] + [vmem] * 6,
        out_specs=(vmem, vmem, vmem),
        scratch_shapes=[
            pltpu.VMEM((2, LE + 2, R + 2 * M + 16, C), F32),
            pltpu.VMEM((2, LE + 2, R + 2 * M + 16, C), F32),
            pltpu.VMEM((SWEEPS, 2, 2, NP, 8, C), F32),
            pltpu.VMEM((SWEEPS, 2, 2, NP, 8, C), F32),
            pltpu.VMEM((S, (R // 2) * C), BF),
            pltpu.VMEM((2, 2 * L, B), F32),
            pltpu.VMEM((2, 2 * L, B), F32),
            pltpu.VMEM((4, G, 128), F32),
            pltpu.VMEM((B // 128, 2 * L, 128), F32),
            pltpu.VMEM((B // 128, 2 * L, 128), F32),
            pltpu.VMEM((B // 128, 2 * L, 128), F32),
            pltpu.VMEM((2, B // 128, L, 128), F32),
            pltpu.VMEM((2, B // 128, L, 128), F32),
            pltpu.VMEM((R // 2, L, C), F32),
            pltpu.VMEM((2, 8, C), F32),
            pltpu.VMEM((2, 8, C), F32),
            pltpu.VMEM((2, L, C), F32),
            pltpu.VMEM((2, L, C), F32),
            pltpu.SemaphoreType.DMA((10,)),
            pltpu.SemaphoreType.DMA((10,)),
            pltpu.SemaphoreType.DMA((SWEEPS, 2, 2)),
            pltpu.SemaphoreType.DMA((SWEEPS, 2, 2)),
            pltpu.SemaphoreType.DMA((6,)),
            pltpu.SemaphoreType.DMA((6,)),
        ],
        compiler_params=pltpu.CompilerParams(collective_id=0, has_side_effects=True),
    )(
        warm, humid, cx, cy, gas[None], drop[None], sw[None], lw[None], flags, slots,
    )
    t, m, rates = pl.pallas_call(
        hand_on,
        out_shape=tuple(jax.ShapeDtypeStruct(a.shape, F32) for a in (t, m, rates)),
        in_specs=[vmem] * 3,
        out_specs=(vmem,) * 3,
    )(t, m, rates)
    return t, m, rates.T


def solution(mesh):
    assert mesh.shape["grp"] == 2
    in_specs = (
        P("grp", "gx", "gy"), P("grp", "gx", "gy"), P(), P(), P(), P(), P(), P(),
        P(("grp", "gx", "gy"), None), P("gx", "gy"),
    )
    out_specs = (P("grp", "gx", "gy"), P("grp", "gx", "gy"), P(("grp", "gx", "gy"), None))
    return jax.shard_map(
        functools.partial(body, mesh.shape["gx"], mesh.shape["gy"]),
        mesh=mesh, in_specs=in_specs, out_specs=out_specs, check_vma=False,
    )
```
